32 devices in a mesh: front: 4 (over z), tile: 8 (over y, x, core).
Axes of the slice: x: 2, y: 2, z: 4, core: 2. Of those that a mesh axis runs over, the one named last changes fastest.
Arguments:
- lower_basis: bfloat16 [4, 8, 512, 1024], P('front', 'tile'), may hold values from -0.75 to 0.75
- lower_coeff: bfloat16 [4, 8, 512, 1024], P('front', 'tile'), may hold values from -0.75 to 0.75
- upper_basis: bfloat16 [4, 8, 512, 1024], P('front', 'tile'), may hold values from -0.75 to 0.75
- upper_coeff: bfloat16 [4, 8, 512, 1024], P('front', 'tile'), may hold values from -0.75 to 0.75
- lower_rank: int32 [4, 8, 32], P('front', 'tile'), may hold values from 1 to 32
- upper_rank: int32 [4, 8, 32], P('front', 'tile'), may hold values from 1 to 32
- child_half: int32 [4, 8], replicated, may hold values from 0 to 1
- owner_shift: int32 [1, 16], replicated, may hold values from 0 to 3
Outputs:
- parent_tiles: bfloat16 [4, 8, 4096, 512], P('front', 'tile')
The draws below stay inside these ranges and needn't reach their ends.
Inputs may be any that keep to these rules, and one draw needn't show every extreme that they name: `child_half`: 0 keeps a tile's index, 1 moves it by 8.
All inputs are finite; a program needn't handle non-finite values.
Results may differ from the reference program's by a relative error of at most 0.0062.
Values may be sent and summed in bfloat16 or wider, within the bound.
A program may use at most 192 MiB of HBM per device.

```python
import jax
import jax.numpy as jnp
from jax import lax

B = 512
R = 32
KP = 32
K = 1024
NC = 8
PT = 16
FRONTS = 4
PARENTS = 1


def touch_ends(entries, own_key, smallest, top_value):
    dims = entries.shape
    index_at = [jax.random.randint(jax.random.fold_in(own_key, axis), (), 0, dims[axis]) for axis in range(len(dims))]
    entries = entries.at[tuple(index_at)].set(smallest)
    longest = dims.index(max(dims))
    index_at[longest] = (index_at[longest] + 1) % dims[longest]
    return entries.at[tuple(index_at)].set(top_value)


def steps_of(key, extent, pieces, low, largest):
    level = 1.0
    for dim, parts in pieces:
        heights = jax.random.uniform(jax.random.fold_in(jax.random.fold_in(key, 6), dim), (parts,), jnp.float32, low / len(pieces), largest / len(pieces))
        level = level * jnp.repeat(jnp.exp(heights), extent[dim] // parts).reshape((-1,) + (1,) * (len(extent) - 1 - dim))
    return level


def bell_draw(stream_key, extent, deviation, limit, cuts=(), kind=jnp.bfloat16):
    drawn = deviation * jax.random.normal(stream_key, extent, jnp.float32)
    if cuts:
        drawn = drawn * steps_of(stream_key, extent, cuts, -0.22, 0.18)
    return jnp.clip(drawn, -limit, limit).astype(kind)


def setup_inputs(seed: int = 0) -> dict:
    keys = jax.random.split(jax.random.key(seed), 9)
    lower_basis = bell_draw(keys[0], (FRONTS, NC, B, K), ((KP * R * R * B) ** -0.125), 0.75, ((0, 4), (1, 8)))
    lower_coeff = bell_draw(keys[1], (FRONTS, NC, B, K), ((KP * R * R * B) ** -0.125), 0.75, ((0, 4), (1, 8)))
    upper_basis = bell_draw(keys[2], (FRONTS, NC, B, K), ((KP * R * R * B) ** -0.125), 0.75, ((0, 4), (1, 8)))
    upper_coeff = bell_draw(keys[3], (FRONTS, NC, B, K), ((KP * R * R * B) ** -0.125), 0.75, ((0, 4), (1, 8)))
    lower_rank = touch_ends(jax.random.randint(keys[4], (FRONTS, NC, KP), 1, R + 1), jax.random.fold_in(keys[4], 1), 1, R).astype(jnp.int32)
    upper_rank = touch_ends(jax.random.randint(keys[5], (FRONTS, NC, KP), 1, R + 1), jax.random.fold_in(keys[5], 1), 1, R).astype(jnp.int32)
    child_half = touch_ends(jax.random.randint(keys[6], (FRONTS, NC), 0, 2), jax.random.fold_in(keys[6], 1), 0, 1).astype(jnp.int32)
    owner_shift = touch_ends(jax.random.randint(keys[7], (PARENTS, PT), 0, 4), jax.random.fold_in(keys[7], 1), 0, 3).astype(jnp.int32)
    return {"lower_basis": lower_basis, "lower_coeff": lower_coeff, "upper_basis": upper_basis, "upper_coeff": upper_coeff, "lower_rank": lower_rank, "upper_rank": upper_rank, "child_half": child_half, "owner_shift": owner_shift}


def masked(basis, ranks):
    keep = (jnp.arange(R, dtype=jnp.int32)[None, None, :] < ranks[:, :, None]).astype(jnp.float32)
    rows = basis.shape[0]
    return basis.astype(jnp.float32).reshape(rows, B, KP, R) * keep[:, None]


def front_tiles(lower_basis, lower_coeff, upper_basis, upper_coeff, lower_rank, upper_rank):
    lower_kept = masked(lower_basis, lower_rank)
    coeff_rows = lower_coeff.astype(jnp.float32).reshape(NC, B, KP, R)

    def column(packed):
        upper_one, coeff_one, col_ranks = packed
        upper_rows = upper_one.astype(jnp.float32).reshape(B, KP, R)
        upper_kept = masked(coeff_one[None], col_ranks[None])[0].reshape(B, KP * R)
        middle = jnp.einsum('ibkr,bks->ikrs', coeff_rows, upper_rows).astype(jnp.bfloat16)
        middle = lax.optimization_barrier(middle).astype(jnp.float32)
        widened = jnp.einsum('ibkr,ikrs->ibks', lower_kept, middle).astype(jnp.bfloat16)
        widened = lax.optimization_barrier(widened).astype(jnp.float32).reshape(NC, B, KP * R)
        return jnp.einsum('ibk,ck->ibc', widened, upper_kept).astype(jnp.bfloat16)

    return lax.map(column, (upper_basis, upper_coeff, upper_rank))


def reference(lower_basis, lower_coeff, upper_basis, upper_coeff, lower_rank, upper_rank, child_half, owner_shift):
    all_tiles = lax.map(lambda packed: front_tiles(*packed),
                        (lower_basis, lower_coeff, upper_basis, upper_coeff, lower_rank, upper_rank))
    half_rows = NC // 2
    col_ids = jnp.arange(NC, dtype=jnp.int32)[:, None]
    slot_ids = jnp.arange(NC, dtype=jnp.int32)[None, :]
    col_half = slot_ids // half_rows
    row_group = slot_ids % half_rows
    parent_col = col_ids + NC * col_half

    def receiver(out_front):
        parent = out_front // 4
        offset = out_front % 4
        shifts = lax.dynamic_index_in_dim(owner_shift, parent, 0, keepdims=False)
        parent_row = 4 * row_group + (offset - shifts[parent_col]) % 4
        child_row = parent_row % NC
        row_half = parent_row // NC
        assembled = jnp.zeros((NC, NC, B, B), jnp.float32)
        for sibling in range(4):
            child_front = 4 * parent + sibling
            tiles = lax.dynamic_index_in_dim(all_tiles, child_front, 0, keepdims=False)
            halves = lax.dynamic_index_in_dim(child_half, child_front, 0, keepdims=False)
            matches = (halves[col_ids] == col_half) & (halves[child_row] == row_half)
            picked = tiles[col_ids, child_row].astype(jnp.float32)
            assembled = assembled + jnp.where(matches[:, :, None, None], picked, jnp.float32(0.0))
        return assembled.astype(jnp.bfloat16).reshape(NC, NC * B, B)

    return lax.map(receiver, jnp.arange(FRONTS, dtype=jnp.int32))
```

```python
import functools

import jax
import jax.numpy as jnp
from jax import lax
from jax.experimental import pallas as pl
from jax.experimental.pallas import tpu as pltpu
from jax.sharding import PartitionSpec as P

MESH = pl.DeviceIdType.MESH
R = 32
YC = 8
XC = 8
LAG = 2
AHEAD = 3
STRIP = 16
LANES = 256
VMEM_OUT = 6 * 2**20
BF16, F32 = jnp.bfloat16, jnp.float32


def rank_mask(rank_ref, columns):
    col = lax.broadcasted_iota(jnp.int32, (8, columns), 1)
    panel, within = col // R, col % R
    rank = jnp.zeros((8, columns), jnp.int32)
    for k in range(columns // R):
        rank = jnp.where(panel == k, rank_ref[0, 0, k], rank)
    return jnp.where(within < rank, 1.0, 0.0).astype(F32)


def schur_kernel(
    n, staged, xb, yb, pb, qb, lr, ur, half_ref, shift_ref, out,
    xbuf, ybuf, pbuf, qbuf, ptbuf, qtbuf, nbuf, tbuf, zbuf, recv, keep_q, obuf,
    load_sem, send_sem, recv_sem, zsend_sem, zrecv_sem, out_sem,
):
    block, columns = xb.shape[2:]
    rows, group = block // XC, columns // YC
    na = n // 4
    front, me = lax.axis_index("front"), lax.axis_index("tile")
    parent, z = front // 4, lax.rem(front, 4)
    a, b, c = me // 4, lax.rem(me // 2, 2), lax.rem(me, 2)
    turn = lax.rem(a - c + na, na)
    sib = me + 1 - 2 * c
    across = me + 2 - 4 * b
    peers = [lax.rem(a - d + na, na) * 4 + b * 2 + c for d in range(1, na)]

    def tile_of(ai, bi, ci):
        return ai * 4 + bi * 2 + ci

    def rows_at(ch):
        return pl.ds(pl.multiple_of(ch * rows, rows), rows)

    def cols_at(j):
        return pl.ds(pl.multiple_of(j * group, group), group)

    def loads():
        return [
            pltpu.make_async_copy(xb.at[0, 0], xbuf.at[me], load_sem.at[0]),
            pltpu.make_async_copy(yb.at[0, 0], ybuf.at[me], load_sem.at[1]),
            pltpu.make_async_copy(pb.at[0, 0], pbuf, load_sem.at[2]),
            pltpu.make_async_copy(qb.at[0, 0], qbuf, load_sem.at[3]),
        ]

    for copy in loads():
        copy.start()

    barrier = pltpu.get_barrier_semaphore()
    for t in [sib, across] + peers:
        pl.semaphore_signal(barrier, inc=1, device_id={"tile": t}, device_id_type=MESH)
    for d in range(1, 4):
        pl.semaphore_signal(
            barrier, inc=1, device_id={"front": parent * 4 + lax.rem(z + d, 4)},
            device_id_type=MESH,
        )
    pl.semaphore_wait(barrier, 2 + len(peers) + 3)

    def send(kind, is_x, item, ch, target, own=False):
        if is_x:
            src = dst = xbuf.at[item, rows_at(ch)]
            s = ch + YC
        else:
            dst = ybuf.at[item, :, cols_at(ch)]
            src = yb.at[0, 0, :, cols_at(ch)] if own else dst
            s = ch
        return pltpu.make_async_remote_copy(
            src_ref=src, dst_ref=dst,
            send_sem=send_sem.at[kind, item, s], recv_sem=recv_sem.at[item, s],
            device_id={"tile": target}, device_id_type=MESH,
        )

    def arrived(is_x, item, ch):
        send(0, is_x, item, ch, sib).wait_recv()

    def loop(count, body):
        def step(i, carry):
            body(i)
            return carry
        lax.fori_loop(0, count, step, 0)

    def chunks(is_x):
        return XC if is_x else YC

    def own_copies(p, is_x, ch, do):
        @pl.when(turn == p)
        def _():
            do(send(1, is_x, me, ch, across, True))
        if p > 0:
            do(send(1 + p, is_x, me, ch, peers[p - 1], True))

    def start(copy):
        copy.start()

    def own_start(p, is_x):
        loop(chunks(is_x), lambda ch: own_copies(p, is_x, ch, start))

    def open_y(j):
        own_copies(0, False, j, start)
        send(0, False, me, j, sib, True).start()

    loop(YC, open_y)
    xcopy, ycopy, pcopy, qcopy = loads()
    xcopy.wait()
    keep_x = rank_mask(lr, columns)[:1]

    def open_x(ch):
        at = rows_at(ch)
        xbuf[me, at] = (xbuf[me, at].astype(F32) * keep_x).astype(BF16)

    loop(XC, open_x)

    def open_x_send(ch):
        own_copies(0, True, ch, start)
        send(0, True, me, ch, sib, True).start()

    loop(XC, open_x_send)
    keep_q[...] = rank_mask(ur, columns)
    col_half = half_ref[front, me]
    shift = shift_ref[parent, me + n * col_half]

    def residue_of(d):
        return lax.rem(z + d - shift + 4, 4)

    second = 3 - 2 * lax.rem(z, 2)
    third = 4 - second

    def zsend(p, d, ch):
        at = rows_at(ch)
        return pltpu.make_async_remote_copy(
            src_ref=zbuf.at[p, d - 1, at], dst_ref=recv.at[z, p, at],
            send_sem=zsend_sem.at[p, d - 1, ch], recv_sem=zrecv_sem.at[p, z, ch],
            device_id={"front": parent * 4 + lax.rem(z + d, 4)}, device_id_type=MESH,
        )

    def zarrived(p, d, ch):
        at = rows_at(ch)
        source = lax.rem(z + d, 4)
        pltpu.make_async_remote_copy(
            src_ref=zbuf.at[p, d - 1, at], dst_ref=recv.at[source, p, at],
            send_sem=zsend_sem.at[p, d - 1, ch], recv_sem=zrecv_sem.at[p, source, ch],
            device_id={"front": parent * 4 + source}, device_id_type=MESH,
        ).wait_recv()

    def near_forward(p, is_x, ch, do, wait):
        near = tile_of(lax.rem(a + p, na), b, c)
        if wait:
            arrived(is_x, near, ch)
        if na == 2:
            @pl.when(lax.rem(a + p, 2) != c)
            def _():
                do(send(1, is_x, near, ch, across))
        do(send(0, is_x, near, ch, sib))

    def far_forward(p, is_x, ch, do, wait):
        far_a = lax.rem(c + p, na)
        far = tile_of(far_a, 1 - b, c)
        if wait:
            arrived(is_x, far, ch)
        if na > 2 or p == 0:
            @pl.when(far_a == a)
            def _():
                for d, t in enumerate(peers):
                    do(send(2 + d, is_x, far, ch, t))
        do(send(0, is_x, far, ch, sib))

    row = lax.broadcasted_iota(jnp.int32, (group, 2 * group), 0) // R
    col = lax.rem(lax.broadcasted_iota(jnp.int32, (group, 2 * group), 1), group) // R
    diagonal = row == col

    def prepare(j):
        at = cols_at(j)
        ptbuf[at, :] = jnp.transpose(pbuf[:, at].astype(F32)).astype(BF16)
        kept = qbuf[:, at].astype(F32) * keep_q[:1, at]
        qtbuf[at, :] = jnp.transpose(kept).astype(BF16)

    def middles(j, first, second_item, slot):
        at = cols_at(j)
        y = jnp.concatenate([ybuf[first, :, at], ybuf[second_item, :, at]], axis=1)
        middle = jnp.dot(ptbuf[at, :], y, preferred_element_type=F32)
        middle = jnp.transpose(jnp.where(diagonal, middle, 0.0)).astype(BF16)
        both = jnp.dot(middle, qtbuf[at, :], preferred_element_type=F32).astype(BF16)
        nbuf[slot, at, :] = both[:group]
        nbuf[slot + 1, at, :] = both[group:]

    for p in range(na):
        near = tile_of(lax.rem(a + p, na), b, c)
        sib_near = tile_of(lax.rem(a + p, na), b, 1 - c)
        far = tile_of(lax.rem(c + p, na), 1 - b, c)
        sib_far = tile_of(lax.rem(1 - c + p, na), 1 - b, 1 - c)
        lag = jnp.where(lax.rem(c + p, na) == a, LAG, 0)
        behind = 0 if p == 0 else 1

        def near_middles(j):
            arrived(False, sib_near, j)
            middles(j, near, sib_near, 0)

        def far_middles(j):
            arrived(False, sib_far, j)
            middles(j, far, sib_far, 2)

        def when_in(i, count, body):
            @pl.when((i >= 0) & (i < count))
            def _():
                body(i)

        if p == 0:
            ycopy.wait()
            pcopy.wait()
            qcopy.wait()

            def open_near(j):
                prepare(j)
                near_middles(j)

            loop(AHEAD, open_near)

        def y_step(j):
            if p > 0:
                when_in(j, YC, lambda i: near_forward(p, False, i, start, True))
            when_in(j - behind, YC, lambda i: far_forward(p, False, i, start, True))
            if p == 0:
                when_in(j + AHEAD, YC, open_near)
            else:
                when_in(j - behind - lag, YC, near_middles)
            when_in(j - behind - lag, YC, far_middles)

        loop(YC + behind + LAG, y_step)

        def process(ch):
            arrived(True, sib_near, ch)
            arrived(True, sib_far, ch)
            at = rows_at(ch)
            for slot, (item, bi, ci) in enumerate(
                [(near, b, c), (sib_near, b, 1 - c), (far, 1 - b, c), (sib_far, 1 - b, 1 - c)]
            ):
                tbuf[bi * 2 + ci] = jnp.dot(
                    xbuf[item, at, :], nbuf[slot], preferred_element_type=F32
                ).astype(BF16)
            for d in (2, second, third):
                zbuf[p, d - 1, at] = tbuf[residue_of(d)]
                zsend(p, d, ch).start()
            recv[z, p, at] = tbuf[residue_of(0)]

        def x_step(ch):
            if p > 0:
                when_in(ch, XC, lambda i: near_forward(p, True, i, start, True))
            when_in(ch - behind, XC, lambda i: far_forward(p, True, i, start, True))
            if p + 1 < na:
                @pl.when(ch == XC - 1 + behind)
                def _():
                    own_start(p + 1, False)
                    own_start(p + 1, True)
            when_in(ch - behind - lag, XC, process)

        loop(XC + behind + LAG, x_step)

    def drain(is_x, ch):
        def wait_send(copy):
            copy.wait_send()
        send(0, is_x, me, ch, sib, True).wait_send()
        for p in range(na):
            own_copies(p, is_x, ch, wait_send)
            if p > 0:
                near_forward(p, is_x, ch, wait_send, False)
            far_forward(p, is_x, ch, wait_send, False)

    loop(YC, lambda ch: drain(False, ch))
    loop(XC, lambda ch: drain(True, ch))

    source = []
    for s in range(4):
        child = 4 * parent + s
        half = half_ref[child, me]
        residue = lax.rem(z - shift_ref[parent, me + n * half] + 4, 4)
        begin = jnp.where(residue // 2 == b, a, lax.rem(residue, 2))
        source.append((
            [lax.rem(q - begin + na, na) for q in range(na)],
            [half * 2 + half_ref[child, 4 * q + residue] for q in range(na)],
        ))

    def assemble(ch):
        for p in range(na):
            for d in range(1, 4):
                zarrived(p, d, ch)

        def strip(i):
            at = pl.ds(pl.multiple_of(ch * rows + i * STRIP, STRIP), STRIP)
            to = pl.ds(pl.multiple_of(i * STRIP, STRIP), STRIP) if staged else at
            target = obuf if staged else out
            for k in range(block // LANES):
                lanes = slice(k * LANES, (k + 1) * LANES)
                held = [
                    [recv[s, p, at, lanes].astype(F32) for p in range(na)] for s in range(4)
                ]
                for q in range(na):
                    picked = []
                    for s, (order, owner) in enumerate(source):
                        tile = held[s][0]
                        for p in range(1, na):
                            tile = jnp.where(order[q] == p, held[s][p], tile)
                        picked.append((tile, owner[q]))
                    for halves in range(4):
                        total = None
                        for tile, own in picked:
                            term = jnp.where(own == halves, tile, 0.0)
                            total = term if total is None else total + term
                        slot = (halves // 2) * (n // 2) + (halves % 2) * na + q
                        target[slot, to, lanes] = total.astype(BF16)

        loop(rows // STRIP, strip)
        if staged:
            copy = pltpu.make_async_copy(obuf, out.at[:, rows_at(ch)], out_sem)
            copy.start()
            copy.wait()

    loop(XC, assemble)

    def zdrain(ch):
        for p in range(na):
            for d in range(1, 4):
                zsend(p, d, ch).wait_send()

    loop(XC, zdrain)


def solution(mesh):
    n = mesh.shape["tile"]
    na = n // 4

    def per_device(xb, yb, pb, qb, lr, ur, half, shift):
        block, columns = xb.shape[2:]
        rows = block // XC
        anywhere = pl.BlockSpec(memory_space=pl.ANY)
        scalars = pl.BlockSpec(memory_space=pltpu.SMEM)
        shape = (n, block, block)
        staged = 2 * n * block * block > VMEM_OUT
        out = pl.pallas_call(
            functools.partial(schur_kernel, n, staged),
            out_shape=jax.ShapeDtypeStruct(shape, BF16) if staged else pltpu.VMEM(shape, BF16),
            in_specs=[anywhere] * 4 + [scalars] * 4,
            out_specs=anywhere if staged else pl.BlockSpec(memory_space=pltpu.VMEM),
            scratch_shapes=[
                pltpu.VMEM((n, block, columns), BF16),
                pltpu.VMEM((n, block, columns), BF16),
                pltpu.VMEM((block, columns), BF16),
                pltpu.VMEM((block, columns), BF16),
                pltpu.VMEM((columns, block), BF16),
                pltpu.VMEM((columns, block), BF16),
                pltpu.VMEM((4, columns, block), BF16),
                pltpu.VMEM((4, rows, block), BF16),
                pltpu.VMEM((na, 3, block, block), BF16),
                pltpu.VMEM((4, na, block, block), BF16),
                pltpu.VMEM((8, columns), F32),
                pltpu.VMEM((n, rows, block) if staged else (1, STRIP, block), BF16),
                pltpu.SemaphoreType.DMA((4,)),
                pltpu.SemaphoreType.DMA((na + 1, n, YC + XC)),
                pltpu.SemaphoreType.DMA((n, YC + XC)),
                pltpu.SemaphoreType.DMA((na, 3, XC)),
                pltpu.SemaphoreType.DMA((na, 4, XC)),
                pltpu.SemaphoreType.DMA,
            ],
            compiler_params=pltpu.CompilerParams(
                collective_id=0, has_side_effects=True,
                vmem_limit_bytes=(63 if staged else 56) * 2**20,
            ),
        )(xb, yb, pb, qb, lr, ur, half, shift)
        return out.reshape(1, 1, n * block, block)

    split = P("front", "tile", None, None)
    ranks = P("front", "tile", None)
    return jax.shard_map(
        per_device, mesh=mesh,
        in_specs=(split, split, split, split, ranks, ranks, P(), P()),
        out_specs=split, check_vma=False,
    )
```

```python
import functools

import jax
import jax.numpy as jnp
from jax import lax
from jax.experimental import pallas as pl
from jax.experimental.pallas import tpu as pltpu
from jax.sharding import PartitionSpec as P

MESH = pl.DeviceIdType.MESH
R = 32
YC = (8, 4)
XC = (8, 4)
LAG = 3
AHEAD = 3
STRIP = 16
LANES = 256
SIB_NEAR, SIB_FAR, FAR, NEAR = range(4)
VMEM_OUT = 6 * 2**20
BF16, F32 = jnp.bfloat16, jnp.float32


def rank_mask(rank_ref, columns):
    col = lax.broadcasted_iota(jnp.int32, (8, columns), 1)
    panel, within = col // R, col % R
    rank = jnp.zeros((8, columns), jnp.int32)
    for k in range(columns // R):
        rank = jnp.where(panel == k, rank_ref[0, 0, k], rank)
    return jnp.where(within < rank, 1.0, 0.0).astype(F32)


def chunks(is_x, p):
    return (XC if is_x else YC)[min(p, 1)]


def schur_kernel(
    n, staged, xb, yb, pb, qb, lr_hbm, ur_hbm, half_hbm, shift_hbm, out,
    xbuf, ybuf, pbuf, qbuf, ptbuf, qtbuf, nbuf, xs, zbuf, recv, keep_q, obuf,
    lr, ur, half_ref, shift_ref,
    load_sem, send_sem, first_sem, recv_sem, zsend_sem, zearly_sem, zlast_sem, know_sem, out_sem,
):
    block, columns = xb.shape[2:]
    na = n // 4
    front, me = lax.axis_index("front"), lax.axis_index("tile")
    parent, z = front // 4, lax.rem(front, 4)
    a, b, c = me // 4, lax.rem(me // 2, 2), lax.rem(me, 2)
    turn = lax.rem(a - c + na, na)
    sib = me + 1 - 2 * c
    across = me + 2 - 4 * b
    peers = [lax.rem(a - d + na, na) * 4 + b * 2 + c for d in range(1, na)]

    def tile_of(ai, bi, ci):
        return ai * 4 + bi * 2 + ci

    def rows_at(p, ch):
        rows = block // chunks(True, p)
        return pl.ds(pl.multiple_of(ch * rows, rows), rows)

    def cols_at(p, j):
        group = columns // chunks(False, p)
        return pl.ds(pl.multiple_of(j * group, group), group)

    def loads():
        pairs = [
            (yb.at[0, 0], ybuf.at[me]), (xb.at[0, 0], xbuf.at[me]), (lr_hbm, lr),
            (pb.at[0, 0], pbuf), (qb.at[0, 0], qbuf), (ur_hbm, ur),
            (half_hbm, half_ref), (shift_hbm, shift_ref),
        ]
        return [
            pltpu.make_async_copy(src, dst, load_sem.at[i])
            for i, (src, dst) in enumerate(pairs)
        ]

    for copy in loads():
        copy.start()

    def greet(sem, axes):
        pl.semaphore_signal(sem, inc=1, device_id=axes, device_id_type=MESH)

    barrier = pltpu.get_barrier_semaphore()
    for t in [sib, across] + peers:
        greet(barrier, {"tile": t})

    @pl.when(z > 0)
    def _():
        greet(barrier, {"front": front - 1})

    @pl.when(z < 3)
    def _():
        greet(barrier, {"front": front + 1})

    ycopy, xcopy, lrcopy, pcopy, qcopy, urcopy, halfcopy, shiftcopy = loads()
    ycopy.wait()
    inner = (z > 0) & (z < 3)
    pl.semaphore_wait(barrier, 3 + len(peers) + jnp.where(inner, 1, 0))

    def send(p, kind, role, is_x, item, ch, target):
        if is_x:
            part = xbuf.at[item] if ch is None else xbuf.at[item, rows_at(p, ch)]
            s = 0 if ch is None else ch + YC[min(p, 1)]
        else:
            part = ybuf.at[item] if ch is None else ybuf.at[item, :, cols_at(p, ch)]
            s = 0 if ch is None else ch
        landed = first_sem.at[role, s] if p == 0 else recv_sem.at[p - 1, role, s]
        return pltpu.make_async_remote_copy(
            src_ref=part, dst_ref=part,
            send_sem=send_sem.at[p, kind, int(is_x)], recv_sem=landed,
            device_id={"tile": target}, device_id_type=MESH,
        )

    def arrived(p, role, is_x, item, ch):
        send(p, 0, role, is_x, item, ch, sib).wait_recv()

    def loop(count, body):
        def step(i, carry):
            body(i)
            return carry
        lax.fori_loop(0, count, step, 0)

    def own_copies(p, is_x, ch, do):
        @pl.when(turn == p)
        def _():
            do(send(p, 1, FAR, is_x, me, ch, across))
        if p > 0:
            do(send(p, 2, NEAR, is_x, me, ch, peers[p - 1]))
        else:
            do(send(p, 0, SIB_NEAR, is_x, me, ch, sib))

    def start(copy):
        copy.start()

    def own_start(p, is_x):
        loop(chunks(is_x, p), lambda ch: own_copies(p, is_x, ch, start))

    own_start(0, False)

    @pl.when(inner)
    def _():
        greet(know_sem.at[0], {"front": front - 1})
        greet(know_sem.at[1], {"front": front + 1})

    xcopy.wait()
    lrcopy.wait()
    keep_x = rank_mask(lr, columns)[:1]

    def open_x(ch):
        at = rows_at(0, ch)
        xbuf[me, at] = (xbuf[me, at].astype(F32) * keep_x).astype(BF16)

    loop(chunks(True, 0), open_x)
    own_start(0, True)
    urcopy.wait()
    halfcopy.wait()
    shiftcopy.wait()
    keep_q[...] = rank_mask(ur, columns)
    col_half = half_ref[front, me]
    shift = shift_ref[parent, me + n * col_half]

    def residue_of(d):
        return lax.rem(z + d - shift + 4, 4)

    second = 3 - 2 * lax.rem(z, 2)
    third = 4 - second

    def zcopy(p, d, ch, source, mine):
        at = rows_at(p, ch)
        landed = zlast_sem.at[mine, ch] if p == na - 1 else zearly_sem.at[mine]
        return pltpu.make_async_remote_copy(
            src_ref=zbuf.at[d - 1, p, at], dst_ref=recv.at[source, p, at],
            send_sem=zsend_sem.at[d - 1], recv_sem=landed,
            device_id={"front": parent * 4 + lax.rem(z + d, 4)}, device_id_type=MESH,
        )

    def whole(d, count, sends):
        ref = zbuf.at[d - 1] if sends else recv.at[lax.rem(z + d, 4), pl.ds(0, count)]
        other = zbuf.at[d - 1, pl.ds(0, count)]
        return pltpu.make_async_remote_copy(
            src_ref=ref if sends else other, dst_ref=ref if not sends else other,
            send_sem=zsend_sem.at[d - 1], recv_sem=zearly_sem.at[d - 1],
            device_id={"front": parent * 4 + lax.rem(z + d, 4)}, device_id_type=MESH,
        )

    def near_forward(p, is_x, ch, do, wait):
        near = tile_of(lax.rem(a + p, na), b, c)
        if wait:
            arrived(p, NEAR, is_x, near, ch)
        if na == 2:
            @pl.when(lax.rem(a + p, 2) != c)
            def _():
                do(send(p, 3, FAR, is_x, near, ch, across))
        do(send(p, 4, SIB_NEAR, is_x, near, ch, sib))

    def far_forward(p, is_x, ch, do, wait):
        far_a = lax.rem(c + p, na)
        far = tile_of(far_a, 1 - b, c)
        if wait:
            arrived(p, FAR, is_x, far, ch)
        if na > 2 or p == 0:
            @pl.when(far_a == a)
            def _():
                for d, t in enumerate(peers):
                    do(send(p, 6 + d, FAR, is_x, far, ch, t))
        do(send(p, 5, SIB_FAR, is_x, far, ch, sib))

    def prepare(j):
        at = cols_at(0, j)
        ptbuf[at, :] = jnp.transpose(pbuf[:, at].astype(F32)).astype(BF16)
        kept = qbuf[:, at].astype(F32) * keep_q[:1, at]
        qtbuf[at, :] = jnp.transpose(kept).astype(BF16)

    def middles(p, j, first, second_item, to_first, to_second):
        at = cols_at(p, j)
        group = columns // chunks(False, p)
        row = lax.broadcasted_iota(jnp.int32, (group, 2 * group), 0) // R
        col = lax.rem(lax.broadcasted_iota(jnp.int32, (group, 2 * group), 1), group) // R
        y = jnp.concatenate([ybuf[first, :, at], ybuf[second_item, :, at]], axis=1)
        middle = jnp.dot(ptbuf[at, :], y, preferred_element_type=F32)
        middle = jnp.transpose(jnp.where(row == col, middle, 0.0)).astype(BF16)
        both = jnp.dot(middle, qtbuf[at, :], preferred_element_type=F32).astype(BF16)
        nbuf[to_first, at, :] = both[:group]
        nbuf[to_second, at, :] = both[group:]

    for p in range(na):
        near = tile_of(lax.rem(a + p, na), b, c)
        sib_near = tile_of(lax.rem(a + p, na), b, 1 - c)
        far = tile_of(lax.rem(c + p, na), 1 - b, c)
        sib_far = tile_of(lax.rem(1 - c + p, na), 1 - b, 1 - c)
        near_at, far_at = b * 2, (1 - b) * 2
        lag = jnp.where(lax.rem(c + p, na) == a, LAG, 0)
        behind = 0 if p == 0 else 1
        yc, xc = chunks(False, p), chunks(True, p)

        def near_middles(j):
            arrived(p, SIB_NEAR, False, sib_near, j)
            middles(p, j, near, sib_near, near_at + c, near_at + 1 - c)

        def far_middles(j):
            arrived(p, SIB_FAR, False, sib_far, j)
            middles(p, j, far, sib_far, far_at + c, far_at + 1 - c)

        def when_in(i, count, body):
            @pl.when((i >= 0) & (i < count))
            def _():
                body(i)

        if p == 0:
            pcopy.wait()
            qcopy.wait()

            def open_near(j):
                prepare(j)
                near_middles(j)

            loop(AHEAD, open_near)

        def y_step(j):
            if p > 0:
                when_in(j, yc, lambda i: near_forward(p, False, i, start, True))
            when_in(j - behind, yc, lambda i: far_forward(p, False, i, start, True))
            if p == 0:
                when_in(j + AHEAD, yc, open_near)
            else:
                when_in(j - behind - lag, yc, near_middles)
            when_in(j - behind - lag, yc, far_middles)

        loop(yc + behind + LAG, y_step)

        if p == 0:
            @pl.when(z < 2)
            def _():
                pl.semaphore_wait(know_sem.at[0], 1)

            @pl.when(z > 1)
            def _():
                pl.semaphore_wait(know_sem.at[1], 1)

            @pl.when(z == 1)
            def _():
                greet(know_sem.at[2], {"front": front - 1})

            @pl.when(z == 2)
            def _():
                greet(know_sem.at[2], {"front": front + 1})

            @pl.when(jnp.logical_not(inner))
            def _():
                pl.semaphore_wait(know_sem.at[2], 1)

        def process(ch):
            arrived(p, SIB_NEAR, True, sib_near, ch)
            arrived(p, SIB_FAR, True, sib_far, ch)
            at = rows_at(p, ch)
            rows = block // xc
            for item, to in [
                (near, near_at + c), (sib_near, near_at + 1 - c),
                (far, far_at + c), (sib_far, far_at + 1 - c),
            ]:
                xs[to, :rows] = xbuf[item, at, :]

            def schur(d):
                residue = residue_of(d)
                return jnp.dot(
                    xs[residue, :rows], nbuf[residue], preferred_element_type=F32
                ).astype(BF16)

            for d in (2, second, third):
                zbuf[d - 1, p, at] = schur(d)
                zcopy(p, d, ch, z, 3 - d).start()
            recv[z, p, at] = schur(0)

        def x_step(ch):
            if p > 0:
                when_in(ch, xc, lambda i: near_forward(p, True, i, start, True))
            when_in(ch - behind, xc, lambda i: far_forward(p, True, i, start, True))
            if p + 1 < na:
                @pl.when(ch == xc - 1 + behind)
                def _():
                    own_start(p + 1, False)
                    own_start(p + 1, True)
            when_in(ch - behind - lag, xc, process)

        loop(xc + behind + LAG, x_step)

    def wait_send(copy):
        copy.wait_send()

    for is_x in (False, True):
        for p in range(na):
            own_copies(p, is_x, None, wait_send)
            if p > 0:
                near_forward(p, is_x, None, wait_send, False)
            far_forward(p, is_x, None, wait_send, False)

    source = []
    for s in range(4):
        child = 4 * parent + s
        half = half_ref[child, me]
        residue = lax.rem(z - shift_ref[parent, me + n * half] + 4, 4)
        begin = jnp.where(residue // 2 == b, a, lax.rem(residue, 2))
        source.append((
            [lax.rem(q - begin + na, na) for q in range(na)],
            [half * 2 + half_ref[child, 4 * q + residue] for q in range(na)],
        ))

    if na > 1:
        for d in range(1, 4):
            whole(d, na - 1, False).wait_recv()
    last = na - 1
    rows = block // chunks(True, last)

    def assemble(ch):
        for d in range(1, 4):
            zcopy(last, d, ch, lax.rem(z + d, 4), d - 1).wait_recv()

        def strip(i):
            at = pl.ds(pl.multiple_of(ch * rows + i * STRIP, STRIP), STRIP)
            to = pl.ds(pl.multiple_of(i * STRIP, STRIP), STRIP) if staged else at
            target = obuf if staged else out
            for k in range(block // LANES):
                lanes = slice(k * LANES, (k + 1) * LANES)
                held = [
                    [recv[s, p, at, lanes].astype(F32) for p in range(na)] for s in range(4)
                ]
                for q in range(na):
                    picked = []
                    for s, (order, owner) in enumerate(source):
                        tile = held[s][0]
                        for p in range(1, na):
                            tile = jnp.where(order[q] == p, held[s][p], tile)
                        picked.append((tile, owner[q]))
                    for halves in range(4):
                        total = None
                        for tile, own in picked:
                            term = jnp.where(own == halves, tile, 0.0)
                            total = term if total is None else total + term
                        slot = (halves // 2) * (n // 2) + (halves % 2) * na + q
                        target[slot, to, lanes] = total.astype(BF16)

        loop(rows // STRIP, strip)
        if staged:
            copy = pltpu.make_async_copy(obuf, out.at[:, rows_at(last, ch)], out_sem)
            copy.start()
            copy.wait()

    loop(chunks(True, last), assemble)
    for d in range(1, 4):
        whole(d, na, True).wait_send()


def solution(mesh):
    n = mesh.shape["tile"]
    na = n // 4

    def per_device(xb, yb, pb, qb, lr, ur, half, shift):
        block, columns = xb.shape[2:]
        last_rows = block // chunks(True, na - 1)
        most_rows = max(block // count for count in XC)
        anywhere = pl.BlockSpec(memory_space=pl.ANY)
        scalars = [pltpu.SMEM(value.shape, value.dtype) for value in (lr, ur, half, shift)]
        shape = (n, block, block)
        staged = 2 * n * block * block > VMEM_OUT
        out = pl.pallas_call(
            functools.partial(schur_kernel, n, staged),
            out_shape=jax.ShapeDtypeStruct(shape, BF16) if staged else pltpu.VMEM(shape, BF16),
            in_specs=[anywhere] * 8,
            out_specs=anywhere if staged else pl.BlockSpec(memory_space=pltpu.VMEM),
            scratch_shapes=[
                pltpu.VMEM((n, block, columns), BF16),
                pltpu.VMEM((n, block, columns), BF16),
                pltpu.VMEM((block, columns), BF16),
                pltpu.VMEM((block, columns), BF16),
                pltpu.VMEM((columns, block), BF16),
                pltpu.VMEM((columns, block), BF16),
                pltpu.VMEM((4, columns, block), BF16),
                pltpu.VMEM((4, most_rows, columns), BF16),
                pltpu.VMEM((3, na, block, block), BF16),
                pltpu.VMEM((4, na, block, block), BF16),
                pltpu.VMEM((8, columns), F32),
                pltpu.VMEM((n, last_rows, block) if staged else (1, STRIP, block), BF16),
                *scalars,
                pltpu.SemaphoreType.DMA((8,)),
                pltpu.SemaphoreType.DMA((na, 5 + na, 2)),
                pltpu.SemaphoreType.DMA((3, YC[0] + XC[0])),
                pltpu.SemaphoreType.DMA((max(na - 1, 1), 4, YC[1] + XC[1])),
                pltpu.SemaphoreType.DMA((3,)),
                pltpu.SemaphoreType.DMA((3,)),
                pltpu.SemaphoreType.DMA((3, chunks(True, na - 1))),
                pltpu.SemaphoreType.REGULAR((3,)),
                pltpu.SemaphoreType.DMA,
            ],
            compiler_params=pltpu.CompilerParams(
                collective_id=0, has_side_effects=True,
                vmem_limit_bytes=(63 if staged else 56) * 2**20,
            ),
        )(xb, yb, pb, qb, lr, ur, half, shift)
        return out.reshape(1, 1, n * block, block)

    split = P("front", "tile", None, None)
    ranks = P("front", "tile", None)
    return jax.shard_map(
        per_device, mesh=mesh,
        in_specs=(split, split, split, split, ranks, ranks, P(), P()),
        out_specs=split, check_vma=False,
    )
```

```python
import functools

import jax
import jax.numpy as jnp
from jax import lax
from jax.experimental import pallas as pl
from jax.experimental.pallas import tpu as pltpu
from jax.sharding import PartitionSpec as P

MESH = pl.DeviceIdType.MESH
R = 32
YC = (8, 8)
XC = (8, 8)
LAG = 3
WINDOW = 4
PACE = 2
ZAHEAD = 3
AHEAD = 3
STRIP = 16
LANES = 256
SIB_NEAR, SIB_FAR, FAR, NEAR = range(4)
VMEM_OUT = 6 * 2**20
BF16, F32 = jnp.bfloat16, jnp.float32


def rank_mask(rank_ref, columns):
    col = lax.broadcasted_iota(jnp.int32, (8, columns), 1)
    panel, within = col // R, col % R
    rank = jnp.zeros((8, columns), jnp.int32)
    for k in range(columns // R):
        rank = jnp.where(panel == k, rank_ref[0, 0, k], rank)
    return jnp.where(within < rank, 1.0, 0.0).astype(F32)


def chunks(is_x, p):
    return (XC if is_x else YC)[min(p, 1)]


def schur_kernel(
    n, staged, xb, yb, pb, qb, lr_hbm, ur_hbm, half_hbm, shift_hbm, out,
    xbuf, ybuf, pbuf, qbuf, ptbuf, qtbuf, nbuf, xs, zbuf, recv, keep_q, obuf,
    lr, ur, half_ref, shift_ref,
    load_sem, send_sem, first_sem, recv_sem, zsend_sem, zearly_sem, zlast_sem, know_sem, out_sem,
):
    block, columns = xb.shape[2:]
    na = n // 4
    front, me = lax.axis_index("front"), lax.axis_index("tile")
    parent, z = front // 4, lax.rem(front, 4)
    a, b, c = me // 4, lax.rem(me // 2, 2), lax.rem(me, 2)
    turn = lax.rem(a - c + na, na)
    sib = me + 1 - 2 * c
    across = me + 2 - 4 * b
    peers = [lax.rem(a - d + na, na) * 4 + b * 2 + c for d in range(1, na)]

    def tile_of(ai, bi, ci):
        return ai * 4 + bi * 2 + ci

    def rows_at(p, ch):
        rows = block // chunks(True, p)
        return pl.ds(pl.multiple_of(ch * rows, rows), rows)

    def cols_at(p, j):
        group = columns // chunks(False, p)
        return pl.ds(pl.multiple_of(j * group, group), group)

    def loads():
        pairs = [
            (yb.at[0, 0], ybuf.at[me]), (xb.at[0, 0], xbuf.at[me]), (lr_hbm, lr),
            (pb.at[0, 0], pbuf), (qb.at[0, 0], qbuf), (ur_hbm, ur),
            (half_hbm, half_ref), (shift_hbm, shift_ref),
        ]
        return [
            pltpu.make_async_copy(src, dst, load_sem.at[i])
            for i, (src, dst) in enumerate(pairs)
        ]

    for copy in loads():
        copy.start()

    def greet(sem, axes):
        pl.semaphore_signal(sem, inc=1, device_id=axes, device_id_type=MESH)

    barrier = pltpu.get_barrier_semaphore()
    for t in [sib, across] + peers:
        greet(barrier, {"tile": t})

    @pl.when(z > 0)
    def _():
        greet(barrier, {"front": front - 1})

    @pl.when(z < 3)
    def _():
        greet(barrier, {"front": front + 1})

    ycopy, xcopy, lrcopy, pcopy, qcopy, urcopy, halfcopy, shiftcopy = loads()
    ycopy.wait()
    inner = (z > 0) & (z < 3)
    pl.semaphore_wait(barrier, 3 + len(peers) + jnp.where(inner, 1, 0))

    def send(p, kind, role, is_x, item, ch, target):
        if is_x:
            part = xbuf.at[item] if ch is None else xbuf.at[item, rows_at(p, ch)]
            s = 0 if ch is None else ch + YC[min(p, 1)]
        else:
            part = ybuf.at[item] if ch is None else ybuf.at[item, :, cols_at(p, ch)]
            s = 0 if ch is None else ch
        landed = first_sem.at[role, s] if p == 0 else recv_sem.at[p - 1, role, s]
        return pltpu.make_async_remote_copy(
            src_ref=part, dst_ref=part,
            send_sem=send_sem.at[p, kind, int(is_x)], recv_sem=landed,
            device_id={"tile": target}, device_id_type=MESH,
        )

    def arrived(p, role, is_x, item, ch):
        send(p, 0, role, is_x, item, ch, sib).wait_recv()

    def loop(count, body):
        def step(i, carry):
            body(i)
            return carry
        lax.fori_loop(0, count, step, 0)

    def own_copies(p, is_x, ch, do):
        @pl.when(turn == p)
        def _():
            do(send(p, 1, FAR, is_x, me, ch, across))
        if p > 0:
            do(send(p, 2, NEAR, is_x, me, ch, peers[p - 1]))

    def start(copy):
        copy.start()

    def when_in(i, count, body):
        @pl.when((i >= 0) & (i < count))
        def _():
            body(i)

    def own_next(p, i):
        yc, xc = chunks(False, p), chunks(True, p)
        when_in(i, yc, lambda ch: own_copies(p, False, ch, start))
        when_in(i - yc, xc, lambda ch: own_copies(p, True, ch, start))
        if p + 1 < na:
            when_in(i - yc - xc, WINDOW, lambda ch: own_copies(p + 1, False, ch, start))

    def own_sib(is_x, ch):
        return send(0, 0, SIB_NEAR, is_x, me, ch, sib)

    loop(WINDOW, lambda ch: own_copies(0, False, ch, start))
    loop(chunks(False, 0), lambda ch: own_sib(False, ch).start())

    @pl.when(inner)
    def _():
        greet(know_sem.at[0], {"front": front - 1})
        greet(know_sem.at[1], {"front": front + 1})

    xcopy.wait()
    lrcopy.wait()
    keep_x = rank_mask(lr, columns)[:1]

    def open_x(ch):
        at = rows_at(0, ch)
        xbuf[me, at] = (xbuf[me, at].astype(F32) * keep_x).astype(BF16)

    loop(chunks(True, 0), open_x)
    loop(chunks(True, 0), lambda ch: own_sib(True, ch).start())
    urcopy.wait()
    halfcopy.wait()
    shiftcopy.wait()
    keep_q[...] = rank_mask(ur, columns)
    col_half = half_ref[front, me]
    shift = shift_ref[parent, me + n * col_half]

    def residue_of(d):
        return lax.rem(z + d - shift + 4, 4)

    second = 3 - 2 * lax.rem(z, 2)
    third = 4 - second

    def zcopy(p, d, ch, source, mine):
        at = rows_at(p, ch)
        landed = zlast_sem.at[mine, ch] if p == na - 1 else zearly_sem.at[mine]
        return pltpu.make_async_remote_copy(
            src_ref=zbuf.at[d - 1, p, at], dst_ref=recv.at[source, p, at],
            send_sem=zsend_sem.at[d - 1], recv_sem=landed,
            device_id={"front": parent * 4 + lax.rem(z + d, 4)}, device_id_type=MESH,
        )

    def whole(d, count, sends):
        ref = zbuf.at[d - 1] if sends else recv.at[lax.rem(z + d, 4), pl.ds(0, count)]
        other = zbuf.at[d - 1, pl.ds(0, count)]
        return pltpu.make_async_remote_copy(
            src_ref=ref if sends else other, dst_ref=ref if not sends else other,
            send_sem=zsend_sem.at[d - 1], recv_sem=zearly_sem.at[d - 1],
            device_id={"front": parent * 4 + lax.rem(z + d, 4)}, device_id_type=MESH,
        )

    def paced(p, i, every, ahead):
        ch = i // every + ahead

        @pl.when((i >= 0) & (lax.rem(i, every) == 0) & (ch < chunks(True, p)))
        def _():
            for d in (2, second, third):
                zcopy(p, d, ch, z, 3 - d).start()

    def near_forward(p, is_x, ch, do, wait):
        near = tile_of(lax.rem(a + p, na), b, c)
        if wait:
            arrived(p, NEAR, is_x, near, ch)
        if na == 2:
            @pl.when(lax.rem(a + p, 2) != c)
            def _():
                do(send(p, 3, FAR, is_x, near, ch, across))
        do(send(p, 4, SIB_NEAR, is_x, near, ch, sib))

    def far_forward(p, is_x, ch, do, wait):
        far_a = lax.rem(c + p, na)
        far = tile_of(far_a, 1 - b, c)
        if wait:
            arrived(p, FAR, is_x, far, ch)
        if na > 2 or p == 0:
            @pl.when(far_a == a)
            def _():
                for d, t in enumerate(peers):
                    do(send(p, 6 + d, FAR, is_x, far, ch, t))
        do(send(p, 5, SIB_FAR, is_x, far, ch, sib))

    def prepare(j):
        at = cols_at(0, j)
        ptbuf[at, :] = jnp.transpose(pbuf[:, at].astype(F32)).astype(BF16)
        kept = qbuf[:, at].astype(F32) * keep_q[:1, at]
        qtbuf[at, :] = jnp.transpose(kept).astype(BF16)

    def middles(p, j, first, second_item, to_first, to_second):
        at = cols_at(p, j)
        group = columns // chunks(False, p)
        row = lax.broadcasted_iota(jnp.int32, (group, 2 * group), 0) // R
        col = lax.rem(lax.broadcasted_iota(jnp.int32, (group, 2 * group), 1), group) // R
        y = jnp.concatenate([ybuf[first, :, at], ybuf[second_item, :, at]], axis=1)
        middle = jnp.dot(ptbuf[at, :], y, preferred_element_type=F32)
        middle = jnp.transpose(jnp.where(row == col, middle, 0.0)).astype(BF16)
        both = jnp.dot(middle, qtbuf[at, :], preferred_element_type=F32).astype(BF16)
        nbuf[to_first, at, :] = both[:group]
        nbuf[to_second, at, :] = both[group:]

    def phase(p):
        near = tile_of(lax.rem(a + p, na), b, c)
        sib_near = tile_of(lax.rem(a + p, na), b, 1 - c)
        far = tile_of(lax.rem(c + p, na), 1 - b, c)
        sib_far = tile_of(lax.rem(1 - c + p, na), 1 - b, 1 - c)
        near_at, far_at = b * 2, (1 - b) * 2
        yc, xc = chunks(False, p), chunks(True, p)

        def near_middles(j):
            arrived(p, SIB_NEAR, False, sib_near, j)
            middles(p, j, near, sib_near, near_at + c, near_at + 1 - c)

        def far_middles(j):
            arrived(p, SIB_FAR, False, sib_far, j)
            middles(p, j, far, sib_far, far_at + c, far_at + 1 - c)

        def process(ch):
            arrived(p, SIB_NEAR, True, sib_near, ch)
            arrived(p, SIB_FAR, True, sib_far, ch)
            at = rows_at(p, ch)
            rows = block // xc
            for item, to in [
                (near, near_at + c), (sib_near, near_at + 1 - c),
                (far, far_at + c), (sib_far, far_at + 1 - c),
            ]:
                xs[to, :rows] = xbuf[item, at, :]

            def schur(d):
                residue = residue_of(d)
                return jnp.dot(
                    xs[residue, :rows], nbuf[residue], preferred_element_type=F32
                ).astype(BF16)

            for d in (2, second, third):
                zbuf[d - 1, p, at] = schur(d)
                if p == na - 1:
                    zcopy(p, d, ch, z, 3 - d).start()
                else:
                    @pl.when(ch == 0)
                    def _():
                        zcopy(p, d, 0, z, 3 - d).start()
            recv[z, p, at] = schur(0)
            if p < na - 1:
                paced(p, ch - 3, 3, 1)

        return near_middles, far_middles, process

    def meet():
        @pl.when(z < 2)
        def _():
            pl.semaphore_wait(know_sem.at[0], 1)

        @pl.when(z > 1)
        def _():
            pl.semaphore_wait(know_sem.at[1], 1)

        @pl.when(z == 1)
        def _():
            greet(know_sem.at[2], {"front": front - 1})

        @pl.when(z == 2)
        def _():
            greet(know_sem.at[2], {"front": front + 1})

        @pl.when(jnp.logical_not(inner))
        def _():
            pl.semaphore_wait(know_sem.at[2], 1)

    phases = [phase(p) for p in range(na)]
    pcopy.wait()
    qcopy.wait()

    def open_near(j):
        prepare(j)
        phases[0][0](j)

    loop(AHEAD, open_near)
    first_lag = jnp.where(a == c, LAG, 0)
    bases = [0]
    for p in range(na):
        bases.append(bases[-1] + chunks(False, p) + chunks(True, p))

    def everything(e):
        for p, base in enumerate(bases[:-1]):
            yc, xc = chunks(False, p), chunks(True, p)
            behind = 0 if p == 0 else 1

            def both(forward, i):
                when_in(i, yc, lambda j: forward(p, False, j, start, True))
                when_in(i - yc, xc, lambda ch: forward(p, True, ch, start, True))

            if p > 0:
                both(near_forward, e - base)
            both(far_forward, e - base - behind)
            when_in(e - base, yc + xc, lambda i: own_next(p, i + WINDOW))
            if p > 0:
                when_in(e - base, yc + xc, lambda i: paced(p - 1, i, PACE, ZAHEAD))
        for p, base in enumerate(bases[:-1]):
            yc, xc = chunks(False, p), chunks(True, p)
            near_middles, far_middles, process = phases[p]
            if p == 0:
                when_in(e + AHEAD, yc, open_near)
            work = e - base - (first_lag if p == 0 else LAG + 1)
            if p > 0:
                when_in(work, yc, near_middles)
            when_in(work, yc, far_middles)
            if p == 0:
                @pl.when(work == yc)
                def _():
                    meet()
            when_in(work - yc, xc, process)

    loop(bases[-1] + LAG + 1, everything)

    def wait_send(copy):
        copy.wait_send()

    for is_x in (False, True):
        own_sib(is_x, None).wait_send()
        for p in range(na):
            own_copies(p, is_x, None, wait_send)
            if p > 0:
                near_forward(p, is_x, None, wait_send, False)
            far_forward(p, is_x, None, wait_send, False)

    source = []
    for s in range(4):
        child = 4 * parent + s
        half = half_ref[child, me]
        residue = lax.rem(z - shift_ref[parent, me + n * half] + 4, 4)
        begin = jnp.where(residue // 2 == b, a, lax.rem(residue, 2))
        source.append((
            [lax.rem(q - begin + na, na) for q in range(na)],
            [half * 2 + half_ref[child, 4 * q + residue] for q in range(na)],
        ))

    if na > 1:
        for d in range(1, 4):
            whole(d, na - 1, False).wait_recv()
    last = na - 1
    rows = block // chunks(True, last)

    def assemble(ch):
        for d in range(1, 4):
            zcopy(last, d, ch, lax.rem(z + d, 4), d - 1).wait_recv()

        def strip(i):
            at = pl.ds(pl.multiple_of(ch * rows + i * STRIP, STRIP), STRIP)
            to = pl.ds(pl.multiple_of(i * STRIP, STRIP), STRIP) if staged else at
            target = obuf if staged else out
            for k in range(block // LANES):
                lanes = slice(k * LANES, (k + 1) * LANES)
                held = [
                    [recv[s, p, at, lanes].astype(F32) for p in range(na)] for s in range(4)
                ]
                for q in range(na):
                    picked = []
                    for s, (order, owner) in enumerate(source):
                        tile = held[s][0]
                        for p in range(1, na):
                            tile = jnp.where(order[q] == p, held[s][p], tile)
                        picked.append((tile, owner[q]))
                    for halves in range(4):
                        total = None
                        for tile, own in picked:
                            term = jnp.where(own == halves, tile, 0.0)
                            total = term if total is None else total + term
                        slot = (halves // 2) * (n // 2) + (halves % 2) * na + q
                        target[slot, to, lanes] = total.astype(BF16)

        loop(rows // STRIP, strip)
        if staged:
            copy = pltpu.make_async_copy(obuf, out.at[:, rows_at(last, ch)], out_sem)
            copy.start()
            copy.wait()

    loop(chunks(True, last), assemble)
    for d in range(1, 4):
        whole(d, na, True).wait_send()


def solution(mesh):
    n = mesh.shape["tile"]
    na = n // 4

    def per_device(xb, yb, pb, qb, lr, ur, half, shift):
        block, columns = xb.shape[2:]
        last_rows = block // chunks(True, na - 1)
        most_rows = max(block // count for count in XC)
        anywhere = pl.BlockSpec(memory_space=pl.ANY)
        scalars = [pltpu.SMEM(value.shape, value.dtype) for value in (lr, ur, half, shift)]
        shape = (n, block, block)
        staged = 2 * n * block * block > VMEM_OUT
        out = pl.pallas_call(
            functools.partial(schur_kernel, n, staged),
            out_shape=jax.ShapeDtypeStruct(shape, BF16) if staged else pltpu.VMEM(shape, BF16),
            in_specs=[anywhere] * 8,
            out_specs=anywhere if staged else pl.BlockSpec(memory_space=pltpu.VMEM),
            scratch_shapes=[
                pltpu.VMEM((n, block, columns), BF16),
                pltpu.VMEM((n, block, columns), BF16),
                pltpu.VMEM((block, columns), BF16),
                pltpu.VMEM((block, columns), BF16),
                pltpu.VMEM((columns, block), BF16),
                pltpu.VMEM((columns, block), BF16),
                pltpu.VMEM((4, columns, block), BF16),
                pltpu.VMEM((4, most_rows, columns), BF16),
                pltpu.VMEM((3, na, block, block), BF16),
                pltpu.VMEM((4, na, block, block), BF16),
                pltpu.VMEM((8, columns), F32),
                pltpu.VMEM((n, last_rows, block) if staged else (1, STRIP, block), BF16),
                *scalars,
                pltpu.SemaphoreType.DMA((8,)),
                pltpu.SemaphoreType.DMA((na, 5 + na, 2)),
                pltpu.SemaphoreType.DMA((3, YC[0] + XC[0])),
                pltpu.SemaphoreType.DMA((max(na - 1, 1), 4, YC[1] + XC[1])),
                pltpu.SemaphoreType.DMA((3,)),
                pltpu.SemaphoreType.DMA((3,)),
                pltpu.SemaphoreType.DMA((3, chunks(True, na - 1))),
                pltpu.SemaphoreType.REGULAR((3,)),
                pltpu.SemaphoreType.DMA,
            ],
            compiler_params=pltpu.CompilerParams(
                collective_id=0, has_side_effects=True,
                vmem_limit_bytes=(63 if staged else 56) * 2**20,
            ),
        )(xb, yb, pb, qb, lr, ur, half, shift)
        return out.reshape(1, 1, n * block, block)

    split = P("front", "tile", None, None)
    ranks = P("front", "tile", None)
    return jax.shard_map(
        per_device, mesh=mesh,
        in_specs=(split, split, split, split, ranks, ranks, P(), P()),
        out_specs=split, check_vma=False,
    )
```

```python
import functools

import jax
import jax.numpy as jnp
from jax import lax
from jax.experimental import pallas as pl
from jax.experimental.pallas import tpu as pltpu
from jax.sharding import PartitionSpec as P

MESH = pl.DeviceIdType.MESH
R = 32
YC = (8, 8)
XC = (8, 8)
LAG = 3
WINDOW = 4
PACE = 2
ZAHEAD = 3
AHEAD = 3
STRIP = 16
LANES = 256
SIB_NEAR, SIB_FAR, FAR, NEAR = range(4)
VMEM_OUT = 6 * 2**20
BF16, F32 = jnp.bfloat16, jnp.float32


def rank_mask(rank_ref, columns):
    col = lax.broadcasted_iota(jnp.int32, (8, columns), 1)
    panel, within = col // R, col % R
    rank = jnp.zeros((8, columns), jnp.int32)
    for k in range(columns // R):
        rank = jnp.where(panel == k, rank_ref[0, 0, k], rank)
    return jnp.where(within < rank, 1.0, 0.0).astype(F32)


def chunks(is_x, p):
    return (XC if is_x else YC)[min(p, 1)]


def schur_kernel(
    n, staged, xb, yb, pb, qb, lr_hbm, ur_hbm, half_hbm, shift_hbm, out,
    xbuf, ybuf, pbuf, qbuf, ptbuf, qtbuf, nbuf, xs, zbuf, recv, keep_q, obuf,
    lr, ur, half_ref, shift_ref,
    load_sem, send_sem, first_sem, recv_sem, zsend_sem, zearly_sem, zlast_sem, know_sem, out_sem,
):
    block, columns = xb.shape[2:]
    na = n // 4
    front, me = lax.axis_index("front"), lax.axis_index("tile")
    parent, z = front // 4, lax.rem(front, 4)
    a, b, c = me // 4, lax.rem(me // 2, 2), lax.rem(me, 2)
    turn = lax.rem(a - c + na, na)
    sib = me + 1 - 2 * c
    across = me + 2 - 4 * b
    peers = [lax.rem(a - d + na, na) * 4 + b * 2 + c for d in range(1, na)]

    def tile_of(ai, bi, ci):
        return ai * 4 + bi * 2 + ci

    def rows_at(p, ch):
        rows = block // chunks(True, p)
        return pl.ds(pl.multiple_of(ch * rows, rows), rows)

    def cols_at(p, j):
        group = columns // chunks(False, p)
        return pl.ds(pl.multiple_of(j * group, group), group)

    def loads():
        pairs = [
            (yb.at[0, 0], ybuf.at[me]), (xb.at[0, 0], xbuf.at[me]), (lr_hbm, lr),
            (pb.at[0, 0], pbuf), (qb.at[0, 0], qbuf), (ur_hbm, ur),
            (half_hbm, half_ref), (shift_hbm, shift_ref),
        ]
        return [
            pltpu.make_async_copy(src, dst, load_sem.at[i])
            for i, (src, dst) in enumerate(pairs)
        ]

    for copy in loads():
        copy.start()

    def greet(sem, axes):
        pl.semaphore_signal(sem, inc=1, device_id=axes, device_id_type=MESH)

    barrier = pltpu.get_barrier_semaphore()
    for t in [sib, across] + peers:
        greet(barrier, {"tile": t})

    @pl.when(z > 0)
    def _():
        greet(barrier, {"front": front - 1})

    @pl.when(z < 3)
    def _():
        greet(barrier, {"front": front + 1})

    ycopy, xcopy, lrcopy, pcopy, qcopy, urcopy, halfcopy, shiftcopy = loads()
    ycopy.wait()
    inner = (z > 0) & (z < 3)
    pl.semaphore_wait(barrier, 3 + len(peers) + jnp.where(inner, 1, 0))

    def send(p, kind, role, is_x, item, ch, target):
        if is_x:
            part = xbuf.at[item] if ch is None else xbuf.at[item, rows_at(p, ch)]
            s = 0 if ch is None else ch + YC[min(p, 1)]
        else:
            part = ybuf.at[item] if ch is None else ybuf.at[item, :, cols_at(p, ch)]
            s = 0 if ch is None else ch
        landed = first_sem.at[role, s] if p == 0 else recv_sem.at[p - 1, role, s]
        return pltpu.make_async_remote_copy(
            src_ref=part, dst_ref=part,
            send_sem=send_sem.at[p, kind, int(is_x)], recv_sem=landed,
            device_id={"tile": target}, device_id_type=MESH,
        )

    def arrived(p, role, is_x, item, ch):
        send(p, 0, role, is_x, item, ch, sib).wait_recv()

    def loop(count, body):
        def step(i, carry):
            body(i)
            return carry
        lax.fori_loop(0, count, step, 0)

    def own_copies(p, is_x, ch, do):
        @pl.when(turn == p)
        def _():
            do(send(p, 1, FAR, is_x, me, ch, across))
        if p > 0:
            do(send(p, 2, NEAR, is_x, me, ch, peers[p - 1]))

    def start(copy):
        copy.start()

    def when_in(i, count, body):
        @pl.when((i >= 0) & (i < count))
        def _():
            body(i)

    def own_next(p, i):
        yc, xc = chunks(False, p), chunks(True, p)
        when_in(i, yc, lambda ch: own_copies(p, False, ch, start))
        when_in(i - yc, xc, lambda ch: own_copies(p, True, ch, start))
        if p + 1 < na:
            when_in(i - yc - xc, WINDOW, lambda ch: own_copies(p + 1, False, ch, start))

    def own_sib(is_x, ch):
        return send(0, 0, SIB_NEAR, is_x, me, ch, sib)

    loop(WINDOW, lambda ch: own_copies(0, False, ch, start))
    loop(chunks(False, 0), lambda ch: own_sib(False, ch).start())

    @pl.when(inner)
    def _():
        greet(know_sem.at[0], {"front": front - 1})
        greet(know_sem.at[1], {"front": front + 1})

    xcopy.wait()
    lrcopy.wait()
    keep_x = rank_mask(lr, columns)[:1]

    def open_x(ch):
        at = rows_at(0, ch)
        xbuf[me, at] = (xbuf[me, at].astype(F32) * keep_x).astype(BF16)

    loop(chunks(True, 0), open_x)
    loop(chunks(True, 0), lambda ch: own_sib(True, ch).start())
    urcopy.wait()
    halfcopy.wait()
    shiftcopy.wait()
    keep_q[...] = rank_mask(ur, columns)
    col_half = half_ref[front, me]
    shift = shift_ref[parent, me + n * col_half]

    def residue_of(d):
        return lax.rem(z + d - shift + 4, 4)

    second = 3 - 2 * lax.rem(z, 2)
    third = 4 - second

    def zcopy(p, d, ch, source, mine):
        at = rows_at(p, ch)
        landed = zlast_sem.at[mine, ch] if p == na - 1 else zearly_sem.at[mine]
        return pltpu.make_async_remote_copy(
            src_ref=zbuf.at[d - 1, p, at], dst_ref=recv.at[source, p, at],
            send_sem=zsend_sem.at[d - 1], recv_sem=landed,
            device_id={"front": parent * 4 + lax.rem(z + d, 4)}, device_id_type=MESH,
        )

    def whole(d, count, sends):
        ref = zbuf.at[d - 1] if sends else recv.at[lax.rem(z + d, 4), pl.ds(0, count)]
        other = zbuf.at[d - 1, pl.ds(0, count)]
        return pltpu.make_async_remote_copy(
            src_ref=ref if sends else other, dst_ref=ref if not sends else other,
            send_sem=zsend_sem.at[d - 1], recv_sem=zearly_sem.at[d - 1],
            device_id={"front": parent * 4 + lax.rem(z + d, 4)}, device_id_type=MESH,
        )

    def paced(p, i, every, ahead):
        ch = i // every + ahead

        @pl.when((i >= 0) & (lax.rem(i, every) == 0) & (ch < chunks(True, p)))
        def _():
            for d in (2, second, third):
                zcopy(p, d, ch, z, 3 - d).start()

    def near_forward(p, is_x, ch, do, wait):
        near = tile_of(lax.rem(a + p, na), b, c)
        if wait:
            arrived(p, NEAR, is_x, near, ch)
        if na == 2:
            @pl.when(lax.rem(a + p, 2) != c)
            def _():
                do(send(p, 3, FAR, is_x, near, ch, across))
        do(send(p, 4, SIB_NEAR, is_x, near, ch, sib))

    def far_forward(p, is_x, ch, do, wait):
        far_a = lax.rem(c + p, na)
        far = tile_of(far_a, 1 - b, c)
        if wait:
            arrived(p, FAR, is_x, far, ch)
        if na > 2 or p == 0:
            @pl.when(far_a == a)
            def _():
                for d, t in enumerate(peers):
                    do(send(p, 6 + d, FAR, is_x, far, ch, t))
        do(send(p, 5, SIB_FAR, is_x, far, ch, sib))

    def prepare(j):
        at = cols_at(0, j)
        ptbuf[at, :] = jnp.transpose(pbuf[:, at].astype(F32)).astype(BF16)
        kept = qbuf[:, at].astype(F32) * keep_q[:1, at]
        qtbuf[at, :] = jnp.transpose(kept).astype(BF16)

    def middles(p, j, first, second_item, to_first, to_second):
        at = cols_at(p, j)
        group = columns // chunks(False, p)
        row = lax.broadcasted_iota(jnp.int32, (group, 2 * group), 0) // R
        col = lax.rem(lax.broadcasted_iota(jnp.int32, (group, 2 * group), 1), group) // R
        y = jnp.concatenate([ybuf[first, :, at], ybuf[second_item, :, at]], axis=1)
        middle = jnp.dot(ptbuf[at, :], y, preferred_element_type=F32)
        middle = jnp.transpose(jnp.where(row == col, middle, 0.0)).astype(BF16)
        both = jnp.dot(middle, qtbuf[at, :], preferred_element_type=F32).astype(BF16)
        nbuf[to_first, at, :] = both[:group]
        nbuf[to_second, at, :] = both[group:]

    def phase(p):
        near = tile_of(lax.rem(a + p, na), b, c)
        sib_near = tile_of(lax.rem(a + p, na), b, 1 - c)
        far = tile_of(lax.rem(c + p, na), 1 - b, c)
        sib_far = tile_of(lax.rem(1 - c + p, na), 1 - b, 1 - c)
        near_at, far_at = b * 2, (1 - b) * 2
        yc, xc = chunks(False, p), chunks(True, p)

        def near_middles(j):
            arrived(p, SIB_NEAR, False, sib_near, j)
            middles(p, j, near, sib_near, near_at + c, near_at + 1 - c)

        def far_middles(j):
            arrived(p, SIB_FAR, False, sib_far, j)
            middles(p, j, far, sib_far, far_at + c, far_at + 1 - c)

        def process(ch):
            arrived(p, SIB_NEAR, True, sib_near, ch)
            arrived(p, SIB_FAR, True, sib_far, ch)
            at = rows_at(p, ch)
            rows = block // xc
            for item, to in [
                (near, near_at + c), (sib_near, near_at + 1 - c),
                (far, far_at + c), (sib_far, far_at + 1 - c),
            ]:
                xs[to, :rows] = xbuf[item, at, :]

            def schur(d):
                residue = residue_of(d)
                return jnp.dot(
                    xs[residue, :rows], nbuf[residue], preferred_element_type=F32
                ).astype(BF16)

            for d in (2, second, third):
                zbuf[d - 1, p, at] = schur(d)
                if p == na - 1:
                    zcopy(p, d, ch, z, 3 - d).start()
                else:
                    @pl.when(ch == 0)
                    def _():
                        zcopy(p, d, 0, z, 3 - d).start()
            recv[z, p, at] = schur(0)
            if p < na - 1:
                paced(p, ch - 3, 3, 1)

        return near_middles, far_middles, process

    def meet():
        @pl.when(z < 2)
        def _():
            pl.semaphore_wait(know_sem.at[0], 1)

        @pl.when(z > 1)
        def _():
            pl.semaphore_wait(know_sem.at[1], 1)

        @pl.when(z == 1)
        def _():
            greet(know_sem.at[2], {"front": front - 1})

        @pl.when(z == 2)
        def _():
            greet(know_sem.at[2], {"front": front + 1})

        @pl.when(jnp.logical_not(inner))
        def _():
            pl.semaphore_wait(know_sem.at[2], 1)

    phases = [phase(p) for p in range(na)]
    pcopy.wait()
    qcopy.wait()

    def open_near(j):
        prepare(j)
        phases[0][0](j)

    loop(AHEAD, open_near)
    first_lag = jnp.where(a == c, LAG, 0)
    bases = [0]
    for p in range(na):
        bases.append(bases[-1] + chunks(False, p) + chunks(True, p))

    def everything(e):
        for p, base in enumerate(bases[:-1]):
            yc, xc = chunks(False, p), chunks(True, p)
            behind = 0 if p == 0 else 1

            def both(forward, i):
                when_in(i, yc, lambda j: forward(p, False, j, start, True))
                when_in(i - yc, xc, lambda ch: forward(p, True, ch, start, True))

            if p > 0:
                both(near_forward, e - base)
            both(far_forward, e - base - behind)
            when_in(e - base, yc + xc, lambda i: own_next(p, i + WINDOW))
            if p > 0:
                when_in(e - base, yc + xc, lambda i: paced(p - 1, i, PACE, ZAHEAD))
        for p, base in enumerate(bases[:-1]):
            yc, xc = chunks(False, p), chunks(True, p)
            near_middles, far_middles, process = phases[p]
            if p == 0:
                when_in(e + AHEAD, yc, open_near)
            work = e - base - (first_lag if p == 0 else LAG)
            if p > 0:
                when_in(work, yc, near_middles)
            when_in(work, yc, far_middles)
            if p == 0:
                @pl.when(work == yc)
                def _():
                    meet()
            when_in(work - yc, xc, process)

    loop(bases[-1] + LAG + 1, everything)

    def wait_send(copy):
        copy.wait_send()

    for is_x in (False, True):
        own_sib(is_x, None).wait_send()
        for p in range(na):
            own_copies(p, is_x, None, wait_send)
            if p > 0:
                near_forward(p, is_x, None, wait_send, False)
            far_forward(p, is_x, None, wait_send, False)

    source = []
    for s in range(4):
        child = 4 * parent + s
        half = half_ref[child, me]
        residue = lax.rem(z - shift_ref[parent, me + n * half] + 4, 4)
        begin = jnp.where(residue // 2 == b, a, lax.rem(residue, 2))
        source.append((
            [lax.rem(q - begin + na, na) for q in range(na)],
            [half * 2 + half_ref[child, 4 * q + residue] for q in range(na)],
        ))

    if na > 1:
        for d in range(1, 4):
            whole(d, na - 1, False).wait_recv()
    last = na - 1
    rows = block // chunks(True, last)

    def assemble(ch):
        for d in range(1, 4):
            zcopy(last, d, ch, lax.rem(z + d, 4), d - 1).wait_recv()

        def strip(i):
            at = pl.ds(pl.multiple_of(ch * rows + i * STRIP, STRIP), STRIP)
            to = pl.ds(pl.multiple_of(i * STRIP, STRIP), STRIP) if staged else at
            target = obuf if staged else out
            for k in range(block // LANES):
                lanes = slice(k * LANES, (k + 1) * LANES)
                held = [
                    [recv[s, p, at, lanes].astype(F32) for p in range(na)] for s in range(4)
                ]
                for q in range(na):
                    picked = []
                    for s, (order, owner) in enumerate(source):
                        tile = held[s][0]
                        for p in range(1, na):
                            tile = jnp.where(order[q] == p, held[s][p], tile)
                        picked.append((tile, owner[q]))
                    for halves in range(4):
                        total = None
                        for tile, own in picked:
                            term = jnp.where(own == halves, tile, 0.0)
                            total = term if total is None else total + term
                        slot = (halves // 2) * (n // 2) + (halves % 2) * na + q
                        target[slot, to, lanes] = total.astype(BF16)

        loop(rows // STRIP, strip)
        if staged:
            copy = pltpu.make_async_copy(obuf, out.at[:, rows_at(last, ch)], out_sem)
            copy.start()
            copy.wait()

    loop(chunks(True, last), assemble)
    for d in range(1, 4):
        whole(d, na, True).wait_send()


def solution(mesh):
    n = mesh.shape["tile"]
    na = n // 4

    def per_device(xb, yb, pb, qb, lr, ur, half, shift):
        block, columns = xb.shape[2:]
        last_rows = block // chunks(True, na - 1)
        most_rows = max(block // count for count in XC)
        anywhere = pl.BlockSpec(memory_space=pl.ANY)
        scalars = [pltpu.SMEM(value.shape, value.dtype) for value in (lr, ur, half, shift)]
        shape = (n, block, block)
        staged = 2 * n * block * block > VMEM_OUT
        out = pl.pallas_call(
            functools.partial(schur_kernel, n, staged),
            out_shape=jax.ShapeDtypeStruct(shape, BF16) if staged else pltpu.VMEM(shape, BF16),
            in_specs=[anywhere] * 8,
            out_specs=anywhere if staged else pl.BlockSpec(memory_space=pltpu.VMEM),
            scratch_shapes=[
                pltpu.VMEM((n, block, columns), BF16),
                pltpu.VMEM((n, block, columns), BF16),
                pltpu.VMEM((block, columns), BF16),
                pltpu.VMEM((block, columns), BF16),
                pltpu.VMEM((columns, block), BF16),
                pltpu.VMEM((columns, block), BF16),
                pltpu.VMEM((4, columns, block), BF16),
                pltpu.VMEM((4, most_rows, columns), BF16),
                pltpu.VMEM((3, na, block, block), BF16),
                pltpu.VMEM((4, na, block, block), BF16),
                pltpu.VMEM((8, columns), F32),
                pltpu.VMEM((n, last_rows, block) if staged else (1, STRIP, block), BF16),
                *scalars,
                pltpu.SemaphoreType.DMA((8,)),
                pltpu.SemaphoreType.DMA((na, 5 + na, 2)),
                pltpu.SemaphoreType.DMA((3, YC[0] + XC[0])),
                pltpu.SemaphoreType.DMA((max(na - 1, 1), 4, YC[1] + XC[1])),
                pltpu.SemaphoreType.DMA((3,)),
                pltpu.SemaphoreType.DMA((3,)),
                pltpu.SemaphoreType.DMA((3, chunks(True, na - 1))),
                pltpu.SemaphoreType.REGULAR((3,)),
                pltpu.SemaphoreType.DMA,
            ],
            compiler_params=pltpu.CompilerParams(
                collective_id=0, has_side_effects=True,
                vmem_limit_bytes=(63 if staged else 56) * 2**20,
            ),
        )(xb, yb, pb, qb, lr, ur, half, shift)
        return out.reshape(1, 1, n * block, block)

    split = P("front", "tile", None, None)
    ranks = P("front", "tile", None)
    return jax.shard_map(
        per_device, mesh=mesh,
        in_specs=(split, split, split, split, ranks, ranks, P(), P()),
        out_specs=split, check_vma=False,
    )
```
